128 devices in a mesh: seg: 4 (over z), cp: 32 (over y, x, core).
Axes of the slice: x: 4, y: 4, z: 4, core: 2. Of those that a mesh axis runs over, the one named last changes fastest.
Arguments:
- mixed_qkv: bfloat16 [16384, 8192], P(('seg', 'cp')), may hold values from -6 to 6
- gate_z: bfloat16 [16384, 4096], P(('seg', 'cp')), may hold values from -6 to 6
- gate_logits: bfloat16 [16384, 64], P(('seg', 'cp')), may hold values from -16 to 4
- block_table: int32 [4, 64], P('seg'), may hold values from 0 to 63, as said below
- conv_weight: float32 [4, 8192], replicated, may hold values from -3 to 3
- a_log: float32 [32], replicated, may hold values from -0.7 to 0.7
- dt_bias: float32 [32], replicated, may hold values from -0.5 to 0.5
- norm_gain: float32 [128], replicated, may hold values from 0.25 to 1.75
Outputs:
- mixed_out: bfloat16 [16384, 4096], P(('seg', 'cp'))
The draws below stay inside these ranges and needn't reach their ends.
Inputs may be any that keep to these rules, and one draw needn't show every extreme that they name: Each row of block_table is a permutation of the numbers 0 to 63; its entries at even positions are below 32, those at odd positions are 32 or more.
All inputs are finite; a program needn't handle non-finite values.
Results may differ from the reference program's by a relative error of at most 0.001.
Values may be sent and summed in bfloat16 or wider, within the bound.
A program may use at most 128 MiB of HBM per device.

```python
import jax
import jax.numpy as jnp
from jax import lax

VALUE_HEADS = 32
KEY_HEADS = 16
HEAD_DIM = 128
CONV = 4
BLOCK = 128
TOK_DEV = 128
SEQUENCE_TOKENS = 16384
N_SEG = 4
N_CP = 32


def draw_gate_logits(key, part):
    random_subkeys = jax.random.split(key, 9)
    slow_share = 0.5
    beta_noise = 0.5 * jax.random.normal(random_subkeys[4], (SEQUENCE_TOKENS, VALUE_HEADS), jnp.float32)
    slow_heads = jax.random.uniform(random_subkeys[0], (VALUE_HEADS,), jnp.float32) < slow_share
    beta_base = jnp.where(slow_heads, jax.random.uniform(random_subkeys[1], (VALUE_HEADS,), jnp.float32, -7.0, -5.0), jax.random.uniform(random_subkeys[2], (VALUE_HEADS,), jnp.float32, -1.0, 2.0))
    decay_base = jnp.where(slow_heads, jax.random.uniform(random_subkeys[3], (VALUE_HEADS,), jnp.float32, -13.0, -11.0), jax.random.uniform(random_subkeys[5], (VALUE_HEADS,), jnp.float32, -4.0, -3.0))
    rows_per_half = TOK_DEV // 2
    group_count = SEQUENCE_TOKENS // rows_per_half
    offsets = jax.random.uniform(random_subkeys[6], (group_count, 1, VALUE_HEADS), jnp.float32, -0.7, 0.7)
    offsets = jnp.broadcast_to(offsets, (group_count, rows_per_half, VALUE_HEADS)).reshape(SEQUENCE_TOKENS, VALUE_HEADS)
    beta_logit = beta_base + beta_noise
    decay_logit_raw = decay_base + offsets + 0.3 * jax.random.normal(random_subkeys[7], (SEQUENCE_TOKENS, VALUE_HEADS), jnp.float32)
    doubling_rows = jax.random.uniform(random_subkeys[8], (SEQUENCE_TOKENS, 1), jnp.float32) < 6.0 / SEQUENCE_TOKENS
    doubling_level = jax.random.uniform(jax.random.fold_in(random_subkeys[8], 7), (SEQUENCE_TOKENS, VALUE_HEADS), jnp.float32, -1.0, 0.0)
    decay_logit_raw = jnp.where(doubling_rows, jnp.maximum(decay_logit_raw, doubling_level), decay_logit_raw)
    joined = jnp.concatenate([beta_logit, decay_logit_raw], axis=1)
    return jnp.clip(joined, -16.0, 4.0).astype(jnp.bfloat16)


def draw_block_table(key, part):
    base = jax.random.fold_in(key, 41)
    first_keys = jax.random.split(jax.random.fold_in(base, 1), N_SEG)
    second_keys = jax.random.split(jax.random.fold_in(base, 2), N_SEG)
    first = jax.vmap(lambda one: jax.random.permutation(one, N_CP))(first_keys).astype(jnp.int32)
    second = jax.vmap(lambda one: jax.random.permutation(one, N_CP))(second_keys).astype(jnp.int32) + N_CP
    return jnp.stack([first, second], axis=-1).reshape(N_SEG, 2 * N_CP).astype(jnp.int32)


def levels(own_key, shape, cuts, least, largest):
    factor_of = 1.0
    for position, blocks in cuts:
        draws = jax.random.uniform(jax.random.fold_in(jax.random.fold_in(own_key, 6), position), (blocks,), jnp.float32, least / len(cuts), largest / len(cuts))
        factor_of = factor_of * jnp.repeat(jnp.exp(draws), shape[position] // blocks).reshape((-1,) + (1,) * (len(shape) - 1 - position))
    return factor_of


def normal_values(own_key, shape, deviation, most, cuts=(), kind=jnp.bfloat16):
    factor_of = levels(own_key, shape, cuts, -0.22, 0.18) if cuts else 1.0
    values = jax.random.normal(own_key, shape, jnp.float32) * deviation * factor_of
    return jnp.minimum(jnp.maximum(values, -most), most).astype(kind)


def setup_inputs(seed: int = 0) -> dict:
    seeds = jax.random.split(jax.random.key(seed), 9)
    return {
        "mixed_qkv": normal_values(seeds[0], (SEQUENCE_TOKENS, 2 * KEY_HEADS * HEAD_DIM + VALUE_HEADS * HEAD_DIM), 1.0, 6.0, ((0, 128),)),
        "gate_z": normal_values(seeds[1], (SEQUENCE_TOKENS, VALUE_HEADS * HEAD_DIM), 1.0, 6.0, ((0, 128),)),
        "gate_logits": draw_gate_logits(jax.random.fold_in(seeds[8], 71), 0),
        "block_table": draw_block_table(jax.random.fold_in(seeds[8], 71), 0),
        "conv_weight": normal_values(seeds[4], (CONV, 2 * KEY_HEADS * HEAD_DIM + VALUE_HEADS * HEAD_DIM), CONV ** -0.5, 3.0, (), jnp.float32),
        "a_log": jnp.clip(jax.random.uniform(seeds[5], (VALUE_HEADS,), jnp.float32, -0.7, 0.7), -0.7, 0.7),
        "dt_bias": jnp.clip(jax.random.uniform(seeds[6], (VALUE_HEADS,), jnp.float32, -0.5, 0.5), -0.5, 0.5),
        "norm_gain": jnp.clip(1.0 + 0.15 * jax.random.normal(seeds[7], (HEAD_DIM,), jnp.float32), 0.25, 1.75),
    }


highest = lax.Precision.HIGHEST

def to_sequence(stored, table):
    columns = stored.shape[1]
    pieces = stored.reshape(N_SEG, 2 * N_CP, TOK_DEV // 2, columns)
    order = jnp.argsort(table, axis=1).astype(jnp.int32)
    picked = jnp.take_along_axis(pieces, order[:, :, None, None], axis=1)
    return picked.reshape(stored.shape[0], columns)

def causal_conv(rows, weights):
    padded = jnp.pad(rows, ((CONV - 1, 0), (0, 0)))
    length = rows.shape[0]
    summed = jnp.zeros(rows.shape, jnp.float32)
    for offset in range(CONV):
        summed = summed + weights[offset] * padded[offset:offset + length].astype(jnp.float32)
    return jax.nn.silu(summed)

def unit_rows(matrix):
    return matrix * lax.rsqrt(lax.optimization_barrier(jnp.sum(matrix * matrix, axis=-1, keepdims=True)) + 1e-06)

def block_terms(queries, key_rows, values, beta_rate, decays):
    cumulative = jnp.cumsum(decays, axis=-1)
    final_sum = cumulative[..., -1:]
    spread = cumulative[..., :, None] - cumulative[..., None, :]
    row_index = lax.broadcasted_iota(jnp.int32, (BLOCK, BLOCK), 0)
    col_index = lax.broadcasted_iota(jnp.int32, (BLOCK, BLOCK), 1)
    strict = row_index > col_index
    inclusive = row_index >= col_index
    strict_decay = jnp.where(strict, jnp.exp(jnp.where(strict, spread, 0.0)), 0.0)
    incl_decay = jnp.where(inclusive, jnp.exp(jnp.where(inclusive, spread, 0.0)), 0.0)
    weighted = key_rows * beta_rate[..., None]
    lower = jnp.einsum('...cd,...ed->...ce', weighted, key_rows, precision=highest) * strict_decay
    system = lower + jnp.eye(BLOCK, dtype=jnp.float32)
    right_side = jnp.concatenate([values * beta_rate[..., None], weighted * jnp.exp(cumulative)[..., None]], axis=-1)
    solved = jax.scipy.linalg.solve_triangular(system, right_side, lower=True, unit_diagonal=True)
    corrected = solved[..., :HEAD_DIM]
    projector = solved[..., HEAD_DIM:]
    key_decay = key_rows * jnp.exp(final_sum - cumulative)[..., None]
    query_decay = queries * jnp.exp(cumulative)[..., None]
    scores = jnp.einsum('...cd,...ed->...ce', queries, key_rows, precision=highest) * incl_decay
    return (corrected, projector, key_decay, query_decay, scores, jnp.exp(final_sum[..., 0]))

def reference(mixed_qkv, gate_z, gate_logits, block_table, conv_weight, a_log, dt_bias, norm_gain):
    seq_qkv = to_sequence(mixed_qkv, block_table)
    seq_z = to_sequence(gate_z, block_table)
    seq_gates = to_sequence(gate_logits, block_table)
    conv_out = causal_conv(seq_qkv, conv_weight)
    length = conv_out.shape[0]
    key_width = KEY_HEADS * HEAD_DIM
    group_size = VALUE_HEADS // KEY_HEADS
    queries = unit_rows(conv_out[:, :key_width].reshape(length, KEY_HEADS, HEAD_DIM)) * HEAD_DIM ** (-0.5)
    key_rows = unit_rows(conv_out[:, key_width:2 * key_width].reshape(length, KEY_HEADS, HEAD_DIM))
    queries = jnp.repeat(queries, group_size, axis=1)
    key_rows = jnp.repeat(key_rows, group_size, axis=1)
    values = conv_out[:, 2 * key_width:].reshape(length, VALUE_HEADS, HEAD_DIM)
    gate_float = seq_gates.astype(jnp.float32)
    beta_rate = jax.nn.sigmoid(gate_float[:, :VALUE_HEADS])
    decays = -jnp.exp(a_log) * jax.nn.softplus(gate_float[:, VALUE_HEADS:] + dt_bias)
    count = length // BLOCK

    def to_blocks(array):
        return array.reshape(count, BLOCK, VALUE_HEADS, HEAD_DIM).transpose(0, 2, 1, 3)

    def to_block_rates(array):
        return array.reshape(count, BLOCK, VALUE_HEADS).transpose(0, 2, 1)

    def block_step(state, pieces):
        query_block, key_block, value_block, beta_block, decay_block = pieces
        corrected, projector, key_decay, query_decay, scores, last_decay = block_terms(query_block, key_block, value_block, beta_block, decay_block)
        new_values = corrected - jnp.einsum('hcd,hde->hce', projector, state, precision=highest)
        outputs = jnp.einsum('hcd,hde->hce', query_decay, state, precision=highest)
        outputs = outputs + jnp.einsum('hce,hev->hcv', scores, new_values, precision=highest)
        state = last_decay[:, None, None] * state + jnp.einsum('hcd,hce->hde', key_decay, new_values, precision=highest)
        return (state, outputs)
    initial = jnp.zeros((VALUE_HEADS, HEAD_DIM, HEAD_DIM), jnp.float32)
    _, blocked = lax.scan(block_step, initial, (to_blocks(queries), to_blocks(key_rows), to_blocks(values), to_block_rates(beta_rate), to_block_rates(decays)))
    core = blocked.transpose(0, 2, 1, 3).reshape(length, VALUE_HEADS, HEAD_DIM)
    gate_values = seq_z.astype(jnp.float32).reshape(length, VALUE_HEADS, HEAD_DIM)
    scale = lax.rsqrt(lax.optimization_barrier(jnp.mean(core * core, axis=-1, keepdims=True)) + 1e-06)
    normed = core * scale * norm_gain * jax.nn.silu(gate_values)
    return normed.reshape(length, VALUE_HEADS * HEAD_DIM).astype(jnp.bfloat16)
```

```python
import functools
import jax
import jax.numpy as jnp
from jax import lax
from jax.experimental import pallas as pl
from jax.experimental.pallas import tpu as pltpu

HEAD_DIM = 128
CONV = 4
BLOCK = 128
HALF = 64
F32 = jnp.float32
BF = jnp.bfloat16
LEVELS = (2, 4, 8, 16, 32, 64)
highest = lax.Precision.HIGHEST


def split(x):
    hi = x.astype(BF)
    return hi, (x - hi.astype(F32)).astype(BF)


def dot(a, b):
    return jnp.dot(a, b, preferred_element_type=F32)


def pair_lhs(parts):
    return jnp.concatenate(parts, axis=1)


def square_rhs(parts):
    row = jnp.concatenate(parts, axis=1)
    return jnp.concatenate([row, row], axis=0)


def mm_square(lhs, rhs):
    wide = dot(lhs, rhs)
    return wide[:, :HEAD_DIM] + wide[:, HEAD_DIM:]


def mm_wide(lhs, wide):
    high, low = split(wide)
    return dot(lhs, jnp.concatenate([high, high], axis=0)) + dot(lhs[:, :HEAD_DIM], low)


def iotas():
    rows = lax.broadcasted_iota(jnp.int32, (BLOCK, BLOCK), 0)
    cols = lax.broadcasted_iota(jnp.int32, (BLOCK, BLOCK), 1)
    return rows, cols


def fill_masks(mask_ref):
    rows, cols = iotas()
    for level, size in enumerate(LEVELS):
        same_pair = (rows // (2 * size)) == (cols // (2 * size))
        apart = (rows // size) > (cols // size)
        mask_ref[level] = jnp.where(same_pair & apart, 1.0, 0.0).astype(BF)


def fill_rates(beta_logit, decay_logit, a_log, dt_bias, beta_ref, cum_ref):
    beta_ref[...] = 1.0 / (1.0 + jnp.exp(-beta_logit))
    shifted = decay_logit + dt_bias
    soft = jnp.maximum(shifted, 0.0) + jnp.log1p(jnp.exp(-jnp.abs(shifted)))
    decays = -jnp.exp(a_log) * soft
    rows, cols = iotas()
    upper = (rows <= cols).astype(F32)
    cum_ref[...] = jnp.dot(decays, upper, preferred_element_type=F32, precision=highest)


def conv_silu(prior, rows, weights):
    padded = jnp.concatenate([prior, rows], axis=0)
    count = rows.shape[0]
    total = weights[CONV - 1 : CONV] * rows
    for offset in range(CONV - 1):
        start = 8 - (CONV - 1) + offset
        total = total + weights[offset : offset + 1] * padded[start : start + count]
    return total / (1.0 + jnp.exp(-total))


def unit_rows(matrix):
    return matrix * lax.rsqrt(jnp.sum(matrix * matrix, axis=-1, keepdims=True) + 1e-06)


def spread_columns(row):
    return jnp.broadcast_to(row, (BLOCK, BLOCK)).T


def scan_step(carried, maps, shifts):
    wide = mm_wide(maps, carried)
    joined = wide + jnp.concatenate([jnp.zeros_like(shifts), shifts], axis=1)
    return joined[:BLOCK], joined[BLOCK:]


GROUP = 8


def staged_terms(chunks, mask_ref, between):
    rows, cols = iotas()
    every = range(len(chunks))
    cum_cols = [spread_columns(c[4]) for c in chunks]
    beta_cols = [spread_columns(c[3]) for c in chunks]
    key_t = [c[1].T for c in chunks]
    between()
    products = [
        mm_square(pair_lhs(split(jnp.concatenate([c[1], c[0]], axis=0))), square_rhs(split(key_t[i])))
        for i, c in enumerate(chunks)
    ]
    between()
    lows, scores, inverses = [], [], []
    for i, c in enumerate(chunks):
        decay = jnp.exp(jnp.where(rows >= cols, cum_cols[i] - c[4], -1e30))
        lower = jnp.where(rows > cols, products[i][:BLOCK] * beta_cols[i] * decay, 0.0)
        scores.append(products[i][BLOCK:] * decay)
        lows.append(split(lower))
        inverses.append(jnp.where(rows == cols, 1.0, jnp.where((rows // 2 == cols // 2), -lower, 0.0)))
    for level in range(len(LEVELS)):
        mask = mask_ref[level]
        parts = [split(inverse) for inverse in inverses]
        mixed = [
            mm_square(pair_lhs((lows[i][0] * mask, lows[i][1] * mask)), square_rhs(parts[i])) for i in every
        ]
        between()
        inverses = [
            inverses[i] - mm_square(pair_lhs(parts[i]), square_rhs(split(mixed[i]))) for i in every
        ]
        between()
    solved, grown = [], []
    for i, c in enumerate(chunks):
        grown.append(jnp.exp(cum_cols[i]))
        right = jnp.concatenate([c[2] * beta_cols[i], c[1] * (beta_cols[i] * grown[i])], axis=1)
        solved.append(mm_wide(pair_lhs(split(inverses[i])), right))
    between()
    maps, shifts = [], []
    for i, c in enumerate(chunks):
        final = c[4][:, BLOCK - 1 : BLOCK]
        key_decay_t = key_t[i] * jnp.exp(final - c[4])
        both = mm_wide(pair_lhs(split(jnp.concatenate([key_decay_t, scores[i]], axis=0))), solved[i])
        eye = jnp.where(rows == cols, jnp.exp(jnp.broadcast_to(final, (BLOCK, BLOCK))), 0.0)
        straight = jnp.concatenate([eye, c[0] * grown[i]], axis=0)
        maps.append(pair_lhs(split(straight - both[:, HEAD_DIM:])))
        shifts.append(both[:, :HEAD_DIM])
    return maps, shifts


from jax.sharding import PartitionSpec as P

VALUE_HEADS = 32
KEY_HEADS = 16
MESH = pl.DeviceIdType.MESH
CP = 32
CHIPS = 16
N_SEG = 4
KEY_WIDTH = KEY_HEADS * HEAD_DIM


def whole_wait(ref, sem):
    pltpu.make_async_copy(ref, ref, sem).wait()


def fused_kernel(
    order_ref, log_ref, bias_ref, mixed_hbm, z_hbm, gates_hbm, weight_hbm, gain_ref, out_hbm,
    mixed_v, z_v, gates_v, w_v, qa, ka, va, qb, kb, vb, zb, gb, tail_out, tail_in, tail_use,
    logit_scr, beta_ref, cum_ref, mask_ref, map_scr, add_scr, seq_scr, u_ref, shift_ref, last_ref,
    state_in, state_out, state_weights, normed,
    stage_sem, own_sem, send_sem, recv_sem,
):
    me = lax.axis_index("cp")
    seg = lax.axis_index("seg")
    core = lax.rem(me, 2)
    chip = me // 2
    slot = core * CHIPS + chip

    def chip_at(step):
        offset = lax.rem(step * 7, 16)
        x = lax.rem(lax.rem(chip, 4) + lax.rem(offset, 4), 4)
        y = lax.rem(chip // 4 + offset // 4, 4)
        return y * 4 + x

    def peer(chip_index, core_index):
        return (seg, chip_index * 2 + core_index)

    stages = [
        pltpu.make_async_copy(mixed_hbm, mixed_v, stage_sem.at[0]),
        pltpu.make_async_copy(gates_hbm, gates_v, stage_sem.at[1]),
        pltpu.make_async_copy(z_hbm, z_v, stage_sem.at[2]),
    ]
    for place, start in enumerate((chip, KEY_HEADS + chip, 2 * KEY_HEADS + me)):
        columns = pl.ds(pl.multiple_of(start * HEAD_DIM, HEAD_DIM), HEAD_DIM)
        stages.append(pltpu.make_async_copy(weight_hbm.at[:, columns], w_v.at[place], stage_sem.at[3 + place]))
    for stage in stages:
        stage.start()

    barrier = pltpu.get_barrier_semaphore()
    for step in range(1, CP):
        pl.semaphore_signal(barrier, inc=1, device_id=(seg, lax.rem(me + step, CP)), device_id_type=MESH)
    for step in (1, N_SEG - 1):
        pl.semaphore_signal(barrier, inc=1, device_id=(lax.rem(seg + step, N_SEG), me), device_id_type=MESH)
    fill_masks(mask_ref)
    tail_use[...] = jnp.zeros_like(tail_use)
    rows, cols = iotas()
    identity = jnp.where(rows == cols, 1.0, 0.0)
    blank = jnp.zeros_like(identity)
    last_ref[...] = jnp.concatenate([identity, blank], axis=1)
    step_map = pair_lhs(split(jnp.concatenate([identity, blank], axis=0)))
    for place in range(GROUP):
        map_scr[place] = step_map
        add_scr[place] = jnp.zeros((2 * BLOCK, HEAD_DIM), F32)
    for stage in stages:
        stage.wait()
    pl.semaphore_wait(barrier, CP + 1)

    def columns_of(start):
        return pl.ds(pl.multiple_of(start * HEAD_DIM, HEAD_DIM), HEAD_DIM)

    def send(src, dst, index, device):
        pltpu.make_async_remote_copy(
            src_ref=src, dst_ref=dst, send_sem=send_sem.at[index], recv_sem=recv_sem.at[index],
            device_id=device, device_id_type=MESH,
        ).start()

    def keep(src, dst, index):
        pltpu.make_async_copy(src, dst, own_sem.at[index]).start()

    def to_heads(body):
        body(chip, 1 - core)

        def one(step, _):
            there = chip_at(step)
            body(there, core)
            body(there, 1 - core)
            return 0

        lax.fori_loop(1, CHIPS, one, 0)

    def to_chips(body):
        def one(step, _):
            body(chip_at(step))
            return 0

        lax.fori_loop(1, CHIPS, one, 0)

    def send_gates(there, there_core):
        head = there * 2 + there_core
        send(gates_v.at[head], gb.at[slot], 0, peer(there, there_core))

    to_heads(send_gates)
    keep(gates_v.at[me], gb.at[slot], 0)

    def send_half(half, qx, kx, vx, base):
        at = pl.ds(half * HALF, HALF)

        def query_key(there):
            send(mixed_v.at[at, columns_of(there)], qx.at[slot], base, peer(there, core))
            send(mixed_v.at[at, columns_of(KEY_HEADS + there)], kx.at[slot], base + 1, peer(there, core))

        def value(there, there_core):
            head = there * 2 + there_core
            send(mixed_v.at[at, columns_of(2 * KEY_HEADS + head)], vx.at[slot], base + 2, peer(there, there_core))

        to_chips(query_key)
        keep(mixed_v.at[at, columns_of(chip)], qx.at[slot], base)
        keep(mixed_v.at[at, columns_of(KEY_HEADS + chip)], kx.at[slot], base + 1)
        to_heads(value)
        keep(mixed_v.at[at, columns_of(2 * KEY_HEADS + me)], vx.at[slot], base + 2)

    send_half(0, qa, ka, va, 1)
    send_half(1, qb, kb, vb, 4)

    def send_z(there, there_core):
        head = there * 2 + there_core
        send(z_v.at[:, columns_of(head)], zb.at[slot], 7, peer(there, there_core))

    to_heads(send_z)
    keep(z_v.at[:, columns_of(me)], zb.at[slot], 7)

    whole_wait(gb.at[pl.ds(0, CP - 1)], recv_sem.at[0])
    whole_wait(gb.at[0], own_sem.at[0])
    lanes = lax.broadcasted_iota(jnp.int32, (2, BLOCK), 1)

    def gate_row(n, _):
        first = gb[order_ref[2 * n]]
        second = gb[order_ref[2 * n + 1]]
        early = jnp.where(lanes < HALF, first, pltpu.roll(second, HALF, 1))
        late = jnp.where(lanes < HALF, pltpu.roll(first, HALF, 1), second)
        logit_scr[n] = jnp.where(n < CHIPS, early, late)
        return 0

    lax.fori_loop(0, CP, gate_row, 0)
    fill_rates(logit_scr[:, 0, :], logit_scr[:, 1, :], log_ref[me], bias_ref[me], beta_ref, cum_ref)

    mine = pl.ds(core * CHIPS, CHIPS)
    theirs = pl.ds((1 - core) * CHIPS, CHIPS)
    partner = peer(chip, 1 - core)

    def forward(qx, kx, base, index):
        for place, ref in enumerate((qx, kx)):
            whole_wait(ref.at[pl.ds(0, CHIPS - 1)], recv_sem.at[base + place])
            whole_wait(ref.at[0], own_sem.at[base + place])
        send(qx.at[mine], qx.at[mine], index, partner)
        send(kx.at[mine], kx.at[mine], index + 1, partner)

    def arrive(qx, kx, vx, base, index):
        whole_wait(vx.at[pl.ds(0, CP - 1)], recv_sem.at[base + 2])
        whole_wait(vx.at[0], own_sem.at[base + 2])
        whole_wait(qx.at[theirs], recv_sem.at[index])
        whole_wait(kx.at[theirs], recv_sem.at[index + 1])

    forward(qa, ka, 1, 8)
    arrive(qa, ka, va, 1, 8)

    groups = CP // GROUP

    def one_scan(group, place, carried):
        carried, outs = scan_step(carried, map_scr[place], add_scr[place])
        n = lax.rem(group * GROUP + place + 1, CP)
        at = pl.ds(pl.multiple_of(n * BLOCK, BLOCK), BLOCK)
        u_ref[at, :] = pair_lhs(split(outs[:, :HEAD_DIM]))
        shift_ref[at, :] = outs[:, HEAD_DIM:]
        return carried

    def gather(group):
        def one(step, _):
            block = lax.rem(group * 2 * GROUP + 1 + step, 2 * CP)
            source = order_ref[block]
            at = pl.ds(pl.multiple_of(step * HALF, HALF), HALF)

            @pl.when(block < CP)
            def _():
                for place, ref in enumerate((qa, ka, va)):
                    seq_scr[place, at, :] = ref[source]

            @pl.when(block >= CP)
            def _():
                for place, ref in enumerate((qb, kb, vb)):
                    seq_scr[place, at, :] = ref[source]

            return 0

        lax.fori_loop(0, 2 * GROUP + 1, one, 0)

    def body(group, _):
        @pl.when(group == 1)
        def _():
            forward(qb, kb, 4, 10)
            arrive(qb, kb, vb, 4, 10)
            source = order_ref[2 * CP - 1]
            for place, ref in enumerate((qb, kb, vb)):
                tail_out[place] = ref[source][HALF - 16 :]

        @pl.when((group == 2) & (seg < N_SEG - 1))
        def _():
            send(tail_out, tail_in, 12, (seg + 1, me))

        @pl.when((group == 3) & (seg > 0))
        def _():
            whole_wait(tail_in, recv_sem.at[12])
            tail_use[...] = tail_in[...]

        gather(group)
        state = {"carried": last_ref[...], "place": 0, "calls": 0}
        before = jnp.maximum(group - 1, 0)

        def between():
            state["calls"] += 1
            if state["calls"] >= 2 and state["place"] < GROUP:
                state["carried"] = one_scan(before, state["place"], state["carried"])
                state["place"] += 1

        chunks = []
        for place in range(GROUP):
            n = lax.rem(group * GROUP + place + 1, CP)
            found = []
            for kind in range(3):
                start = HALF + place * BLOCK
                block = seq_scr[kind, start - 16 : start + BLOCK, :].astype(F32)
                prior = block[8:16]
                if place == GROUP - 1:
                    prior = jnp.where(n == 0, tail_use[kind].astype(F32)[8:], prior)
                found.append(conv_silu(prior, block[16:], w_v[kind]))
            chunks.append((
                unit_rows(found[0]) * HEAD_DIM ** (-0.5), unit_rows(found[1]), found[2],
                beta_ref[pl.ds(n, 1), :], cum_ref[pl.ds(n, 1), :],
            ))
        maps, shifts = staged_terms(chunks, mask_ref, between)
        for place in range(GROUP):
            map_scr[place] = maps[place]
            add_scr[place] = shifts[place]
        last_ref[...] = state["carried"]
        return 0

    lax.fori_loop(0, groups, body, 0)
    carried = last_ref[...]
    for place in range(GROUP - 1):
        carried = one_scan(groups - 1, place, carried)
    first_map, first_add = map_scr[GROUP - 1], add_scr[GROUP - 1]
    u_ref[0:BLOCK, :] = first_map[BLOCK:]
    shift_ref[0:BLOCK, :] = first_add[BLOCK:]
    first_high, first_low = first_map[:BLOCK, :HEAD_DIM], first_map[:BLOCK, HEAD_DIM:]
    start_map = first_high.astype(F32) + first_low.astype(F32)
    joined = mm_wide(pair_lhs(split(carried[:, :HEAD_DIM])), jnp.concatenate([start_map, first_add[:BLOCK]], axis=1))
    total_map = pair_lhs(split(joined[:, :HEAD_DIM]))
    total_add = joined[:, HEAD_DIM:] + carried[:, HEAD_DIM:]

    @pl.when(seg == 0)
    def _():
        state_in[...] = jnp.zeros_like(state_in)

    @pl.when(seg > 0)
    def _():
        whole_wait(state_in, recv_sem.at[13])

    incoming = square_rhs(split(state_in[...]))
    state_out[...] = mm_square(total_map, incoming) + total_add

    @pl.when(seg < N_SEG - 1)
    def _():
        send(state_out, state_in, 13, (seg + 1, me))

    state_weights[0] = incoming
    state_weights[1] = square_rhs(split(mm_square(first_map[:BLOCK], incoming) + first_add[:BLOCK]))
    whole_wait(zb.at[pl.ds(0, CP - 1)], recv_sem.at[7])
    whole_wait(zb.at[0], own_sem.at[7])

    def finish(n):
        at = pl.ds(pl.multiple_of(n * BLOCK, BLOCK), BLOCK)
        core_rows = mm_square(u_ref[at, :], state_weights[jnp.minimum(n, 1)]) + shift_ref[at, :]
        half = pl.ds(pl.multiple_of((n // CHIPS) * HALF, HALF), HALF)
        gate = jnp.concatenate([zb[order_ref[2 * n], half, :], zb[order_ref[2 * n + 1], half, :]], axis=0).astype(F32)
        scale = lax.rsqrt(jnp.mean(core_rows * core_rows, axis=-1, keepdims=True) + 1e-06)
        normed[n] = (core_rows * scale * gain_ref[...] * (gate / (1.0 + jnp.exp(-gate)))).astype(BF)

    here = out_hbm.at[:, columns_of(me)]

    def finish_chip(step, _):
        there = chip_at(step)
        finish(there * 2)
        finish(there * 2 + 1)

        @pl.when(step > 0)
        def _():
            send(normed.at[there * 2], here, 14, (seg, there * 2))
            send(normed.at[there * 2 + 1], here, 14, (seg, there * 2 + 1))

        return 0

    lax.fori_loop(1, CHIPS + 1, lambda step, c: finish_chip(lax.rem(step, CHIPS), c), 0)
    send(normed.at[chip * 2 + 1 - core], here, 14, partner)
    keep(normed.at[me], here, 14)

    def drain(ref, count, index):
        whole_wait(ref.at[pl.ds(0, count)], send_sem.at[index])

    drain(gb, CP - 1, 0)
    for base, qx, kx, vx, index in ((1, qa, ka, va, 8), (4, qb, kb, vb, 10)):
        drain(qx, CHIPS - 1, base)
        drain(kx, CHIPS - 1, base + 1)
        drain(vx, CP - 1, base + 2)
        drain(qx, CHIPS, index)
        drain(kx, CHIPS, index + 1)
    drain(zb, CP - 1, 7)

    @pl.when(seg < N_SEG - 1)
    def _():
        whole_wait(tail_out, send_sem.at[12])
        whole_wait(state_out, send_sem.at[13])

    drain(normed, CP - 1, 14)
    whole_wait(normed.at[pl.ds(0, CP - 1)], recv_sem.at[14])
    whole_wait(normed.at[0], own_sem.at[14])


VM = pl.BlockSpec(memory_space=pltpu.VMEM)
SM = pl.BlockSpec(memory_space=pltpu.SMEM)
ANY = pl.BlockSpec(memory_space=pl.ANY)
SEMS = 15


def fused_call(order, a_log, dt_bias, mixed, z, gates, weights, gain):
    tokens = CP * BLOCK
    half = pltpu.VMEM((CP, HALF, HEAD_DIM), BF)
    return pl.pallas_call(
        fused_kernel,
        out_shape=jax.ShapeDtypeStruct(z.shape, BF),
        in_specs=[SM, SM, SM, ANY, ANY, ANY, ANY, VM],
        out_specs=ANY,
        scratch_shapes=[
            pltpu.VMEM(mixed.shape, BF),
            pltpu.VMEM(z.shape, BF),
            pltpu.VMEM(gates.shape, F32),
            pltpu.VMEM((3, CONV, HEAD_DIM), F32),
            half, half, half, half, half, half,
            pltpu.VMEM((CP, BLOCK, HEAD_DIM), BF),
            pltpu.VMEM((CP, 2, BLOCK), F32),
            pltpu.VMEM((3, 16, HEAD_DIM), BF),
            pltpu.VMEM((3, 16, HEAD_DIM), BF),
            pltpu.VMEM((3, 16, HEAD_DIM), BF),
            pltpu.VMEM((CP, 2, BLOCK), F32),
            pltpu.VMEM((CP, BLOCK), F32),
            pltpu.VMEM((CP, BLOCK), F32),
            pltpu.VMEM((len(LEVELS), BLOCK, BLOCK), BF),
            pltpu.VMEM((GROUP, 2 * BLOCK, 2 * HEAD_DIM), BF),
            pltpu.VMEM((GROUP, 2 * BLOCK, HEAD_DIM), F32),
            pltpu.VMEM((3, HALF + GROUP * BLOCK, HEAD_DIM), BF),
            pltpu.VMEM((tokens, 2 * HEAD_DIM), BF),
            pltpu.VMEM((tokens, HEAD_DIM), F32),
            pltpu.VMEM((HEAD_DIM, 2 * HEAD_DIM), F32),
            pltpu.VMEM((HEAD_DIM, HEAD_DIM), F32),
            pltpu.VMEM((HEAD_DIM, HEAD_DIM), F32),
            pltpu.VMEM((2, 2 * HEAD_DIM, 2 * HEAD_DIM), BF),
            pltpu.VMEM((CP, BLOCK, HEAD_DIM), BF),
            pltpu.SemaphoreType.DMA((6,)),
            pltpu.SemaphoreType.DMA((SEMS,)),
            pltpu.SemaphoreType.DMA((SEMS,)),
            pltpu.SemaphoreType.DMA((SEMS,)),
        ],
        compiler_params=pltpu.CompilerParams(collective_id=0, has_side_effects=True),
        name="mixer",
    )(order, a_log, dt_bias, mixed, z, gates, weights, gain)


def per_device(mixed_qkv, gate_z, gate_logits, block_table, conv_weight, a_log, dt_bias, norm_gain):
    places = jnp.arange(2 * CP, dtype=jnp.int32) // 2
    slots = (places % 2) * CHIPS + places // 2
    hit = block_table[0][None, :] == jnp.arange(2 * CP, dtype=jnp.int32)[:, None]
    order = jnp.sum(jnp.where(hit, slots[None, :], 0), axis=1)
    gates = gate_logits.astype(F32).reshape(BLOCK, 2, VALUE_HEADS).transpose(2, 1, 0)
    return fused_call(order, a_log, dt_bias, mixed_qkv, gate_z, gates, conv_weight, norm_gain.reshape(1, HEAD_DIM))


def solution(mesh):
    return jax.shard_map(
        per_device,
        mesh=mesh,
        in_specs=(
            P(("seg", "cp"), None), P(("seg", "cp"), None), P(("seg", "cp"), None), P("seg", None),
            P(), P(), P(), P(),
        ),
        out_specs=P(("seg", "cp"), None),
        check_vma=False,
    )
```
